32 devices in a mesh: rep: 4 (over x, core), dp: 4 (over z), tp: 2 (over y).
Axes of the slice: x: 2, y: 2, z: 4, core: 2. Of those that a mesh axis runs over, the one named last changes fastest.
Arguments:
- hidden: bfloat16 [4, 512, 14336], P('rep', None, 'tp'), may hold values from -6 to 6
- down_weight: bfloat16 [14336, 8192], P('tp', 'dp'), may hold values from -0.046875 to 0.046875
- out_grad: bfloat16 [4, 512, 8192], P('rep', 'tp', 'dp'), may hold values from -6 to 6
- pseudo_grad: bfloat16 [4, 14336, 8192], P('rep', 'tp', 'dp'), may hold values from -6 to 6
- momentum: float32 [14336, 8192], P(('tp', 'rep'), 'dp'), may hold values from -6 to 6
Outputs:
- layer_out: bfloat16 [4, 512, 8192], P('rep', 'tp', 'dp')
- hidden_grad: bfloat16 [4, 512, 14336], P('rep', 'dp', 'tp')
- new_momentum: float32 [14336, 8192], P(('tp', 'rep'), 'dp')
- outer_step: bfloat16 [14336, 8192], P('tp', 'dp')
The draws below stay inside these ranges and needn't reach their ends.
All inputs are finite; a program needn't handle non-finite values.
Results may differ from the reference program's by a relative error of at most 0.017.
Values may be sent and summed in bfloat16 or wider, within the bound.
A program may use at most 256 MiB of HBM per device.

```python
import jax
import jax.numpy as jnp
from jax import lax

D = 8192
FF = 14336
TOKENS = 512
N_REP = 4
N_DP = 4
N_TP = 2


def block_scale(key, extent, cuts, low, largest):
    gain = 1.0
    for axis_at, parts in cuts:
        heights = jax.random.uniform(jax.random.fold_in(jax.random.fold_in(key, 6), axis_at), (parts,), jnp.float32, low / len(cuts), largest / len(cuts))
        gain = gain * jnp.repeat(jnp.exp(heights), extent[axis_at] // parts).reshape((-1,) + (1,) * (len(extent) - 1 - axis_at))
    return gain


def bell_draw(rng, dims, spread, reach, cuts=(), kind=jnp.bfloat16):
    level = block_scale(rng, dims, cuts, -0.22, 0.18) if cuts else 1.0
    array = jax.random.normal(rng, dims, jnp.float32) * spread * level
    return jnp.minimum(jnp.maximum(array, -reach), reach).astype(kind)


def setup_inputs(seed: int = 0) -> dict:
    key_list = jax.random.split(jax.random.key(seed), 6)
    return {
        "hidden": bell_draw(key_list[0], (N_REP, TOKENS, FF), 1.0, 6.0, ((0, 4), (2, 2))),
        "down_weight": bell_draw(key_list[1], (FF, D), FF ** -0.5, 0.046875, ((0, 2), (1, 4))),
        "out_grad": bell_draw(key_list[2], (N_REP, TOKENS, D), 1.0, 6.0, ((0, 4), (1, 2), (2, 4))),
        "pseudo_grad": bell_draw(key_list[3], (N_REP, FF, D), 1.0, 6.0, ((0, 4), (1, 2), (2, 4))),
        "momentum": bell_draw(key_list[4], (FF, D), 1.0, 6.0, ((0, 8), (1, 4)), jnp.float32),
    }


outer_rate = 0.7
momentum_rate = 0.9


def reference(hidden, down_weight, out_grad, pseudo_grad, momentum):
    hidden_width = FF // N_TP
    model_width = D // N_DP
    weight_tp = down_weight.reshape(N_TP, hidden_width, D)
    weight_dp = jnp.transpose(down_weight.reshape(FF, N_DP, model_width), (1, 0, 2))

    def forward_block(paired):
        return jnp.dot(paired[0], paired[1], preferred_element_type=jnp.float32).astype(jnp.bfloat16)

    def backward_block(paired):
        product = lax.dot_general(paired[0], paired[1], (((1,), (1,)), ((), ())), preferred_element_type=jnp.float32)
        return product.astype(jnp.bfloat16)

    def one_replica(paired):
        token_rows = paired[0]
        grad_rows = paired[1]
        rows_tp = jnp.transpose(token_rows.reshape(TOKENS, N_TP, hidden_width), (1, 0, 2))
        partial_out = lax.map(forward_block, (rows_tp, weight_tp))
        layer = jnp.sum(partial_out.astype(jnp.float32), axis=0).astype(jnp.bfloat16)
        grads_dp = jnp.transpose(grad_rows.reshape(TOKENS, N_DP, model_width), (1, 0, 2))
        partial_back = lax.map(backward_block, (grads_dp, weight_dp))
        back = jnp.sum(partial_back.astype(jnp.float32), axis=0).astype(jnp.bfloat16)
        return layer, back

    layer_out, hidden_grad = lax.map(one_replica, (hidden, out_grad))

    def accumulate(index, running_sum):
        return running_sum + pseudo_grad[index].astype(jnp.float32)

    totals = lax.fori_loop(0, N_REP, accumulate, jnp.zeros((FF, D), jnp.float32))
    average = totals / N_REP
    new_momentum = momentum_rate * momentum + average
    outer_step = (outer_rate * (average + momentum_rate * new_momentum)).astype(jnp.bfloat16)
    return layer_out, hidden_grad, new_momentum, outer_step
```

```python
import functools

import jax
import jax.numpy as jnp
from jax import lax
from jax.experimental import pallas as pl
from jax.experimental.pallas import tpu as pltpu
from jax.sharding import PartitionSpec as P

outer_rate = 0.7
momentum_rate = 0.9

MESH = pl.DeviceIdType.MESH
f32 = jnp.float32
bf16 = jnp.bfloat16


def pieces(extent, unit, most):
    return max(k for k in range(1, most + 1) if extent % (k * unit) == 0)


def kernel(
    n_rep, n_dp, n_tp, n_k, n_f,
    hidden, weight, grads, pseudo, momentum,
    layer_out, hidden_grad, new_momentum, outer_step, xch,
    ps, pr, la, lb, mom, nmb, wb, hb, gf, acc, po, tr, pb, dr,
    ld_sem, xs_sem, xr_sem, ps_sem, pr_sem, ss_sem, sr_sem, fs_sem, fr_sem, own_sem,
    gs_sem, gr_sem, ts_sem, tr_sem, ds_sem, dr_sem,
):
    n_x = n_rep // 2
    rep, dp, tp = lax.axis_index("rep"), lax.axis_index("dp"), lax.axis_index("tp")
    x, core = rep // 2, lax.rem(rep, 2)
    partner = 2 * x + 1 - core
    share, cols = momentum.shape
    chunk = share // n_k
    ffn = weight.shape[0]
    fb = ffn // n_f
    tokens = hidden.shape[1]
    t_rows, d_rows = tokens // n_tp, tokens // n_dp
    row_unit = 16

    def chip(d):
        return lax.rem(x + d, n_x)

    def rep_peer(d):
        return 2 * chip(d) + core

    def rows(owner, k):
        return pl.ds(pl.multiple_of(owner * share + k * chunk, chunk), chunk)

    def part(k):
        return pl.ds(pl.multiple_of(k * chunk, chunk), chunk)

    def remote(src, dst, send, recv, axis, index):
        return pltpu.make_async_remote_copy(
            src_ref=src, dst_ref=dst, send_sem=send, recv_sem=recv,
            device_id={axis: index}, device_id_type=MESH,
        )

    def drain(ref, sem):
        pltpu.make_async_copy(ref, ref, sem).wait()

    barrier = pltpu.get_barrier_semaphore()
    peers = [("rep", partner)]
    peers += [("rep", rep_peer(d)) for d in range(1, n_x)]
    peers += [("dp", lax.rem(dp + d, n_dp)) for d in range(1, n_dp)]
    peers += [("tp", lax.rem(tp + d, n_tp)) for d in range(1, n_tp)]
    for axis, index in peers:
        pl.semaphore_signal(barrier, inc=1, device_id={axis: index}, device_id_type=MESH)
    pl.semaphore_wait(barrier, len(peers))

    def exchange(d, k):
        return remote(
            pseudo.at[0, rows(2 * chip(d) + 1 - core, k)], xch.at[d, part(k)],
            xs_sem, xr_sem.at[d, k], "rep", partner,
        )

    def start_exchange(k, carry):
        for d in range(1, n_x):
            exchange(d, k).start()
        return carry

    def start_own_exchange(k, carry):
        exchange(0, k).start()
        return carry

    lax.fori_loop(0, n_k, start_exchange, 0)

    mine = pl.ds(pl.multiple_of(tp * t_rows, t_rows), t_rows)

    def gather(d):
        return remote(grads.at[0], gf.at[mine], gs_sem.at[d - 1], gr_sem.at[d - 1],
                      "tp", lax.rem(tp + d, n_tp))

    for d in range(1, n_tp):
        gather(d).start()
    own_grads = pltpu.make_async_copy(grads.at[0], gf.at[mine], own_sem)
    own_grads.start()
    lax.fori_loop(0, n_k, start_own_exchange, 0)

    def partial_send(d, k):
        return remote(ps.at[d - 1, part(k)], pr.at[d - 1, part(k)], ps_sem,
                      pr_sem.at[d - 1, k], "rep", rep_peer(d))

    def reduce_chunk(k, carry):
        for d in range(1, n_x):
            a = pltpu.make_async_copy(pseudo.at[0, rows(rep_peer(d), k)], la, ld_sem.at[0])
            a.start()
            exchange(d, k).wait_recv()
            b = pltpu.make_async_copy(xch.at[d, part(k)], lb, ld_sem.at[1])
            b.start()
            a.wait()
            b.wait()

            def add(i, c):
                r = pl.ds(pl.multiple_of(i * row_unit, row_unit), row_unit)
                o = pl.ds(pl.multiple_of(k * chunk + i * row_unit, row_unit), row_unit)
                ps[d - 1, o, :] = (la[r, :].astype(f32) + lb[r, :].astype(f32)).astype(bf16)
                return c

            lax.fori_loop(0, chunk // row_unit, add, 0)
            partial_send(d, k).start()
        return carry

    lax.fori_loop(0, n_k, reduce_chunk, 0)

    tn = cols // pieces(cols, 128, max(1, cols // 512))
    tm = tokens // pieces(tokens, row_unit, 2)

    def clear(i, carry):
        r = pl.ds(pl.multiple_of(i * row_unit, row_unit), row_unit)
        acc[r, :] = jnp.zeros((row_unit, cols), f32)
        return carry

    lax.fori_loop(0, tokens // row_unit, clear, 0)
    own_grads.wait()
    for d in range(1, n_tp):
        gather(d).wait()

    def back_send(d, f):
        to = lax.rem(dp + d, n_dp)
        c = pl.ds(pl.multiple_of(f * fb, fb), fb)
        return remote(
            pb.at[pl.ds(pl.multiple_of(to * d_rows, d_rows), d_rows), c],
            dr.at[d - 1, :, c], ds_sem, dr_sem.at[d - 1], "dp", to,
        )

    def matmul_block(f, carry):
        c = pl.ds(pl.multiple_of(f * fb, fb), fb)
        a = pltpu.make_async_copy(weight.at[c], wb, ld_sem.at[0])
        b = pltpu.make_async_copy(hidden.at[0, :, c], hb, ld_sem.at[1])
        a.start()
        b.start()
        a.wait()
        b.wait()

        def back(m, z):
            r = pl.ds(pl.multiple_of(m * tm, tm), tm)
            product = lax.dot_general(
                gf[r, :], wb[...], (((1,), (1,)), ((), ())), preferred_element_type=f32
            )
            pb[r, c] = product.astype(bf16)
            return z

        lax.fori_loop(0, tokens // tm, back, 0)
        for d in range(1, n_dp):
            back_send(d, f).start()

        def forward(n, z):
            t = pl.ds(pl.multiple_of(n * tn, tn), tn)
            acc[:, t] += jnp.dot(hb[...], wb[:, t], preferred_element_type=f32)
            return z

        lax.fori_loop(0, cols // tn, forward, 0)
        return carry

    lax.fori_loop(0, n_f, matmul_block, 0)

    def round_out(i, carry):
        r = pl.ds(pl.multiple_of(i * row_unit, row_unit), row_unit)
        po[r, :] = acc[r, :].astype(bf16)
        return carry

    lax.fori_loop(0, tokens // row_unit, round_out, 0)

    def out_send(d):
        to = lax.rem(tp + d, n_tp)
        return remote(po.at[pl.ds(pl.multiple_of(to * t_rows, t_rows), t_rows)],
                      tr.at[d - 1], ts_sem.at[d - 1], tr_sem.at[d - 1], "tp", to)

    for d in range(1, n_tp):
        out_send(d).start()

    def store_momentum(k):
        return pltpu.make_async_copy(nmb, new_momentum.at[part(k)], ld_sem.at[3])

    def step_send(d, k):
        return remote(pr.at[0, part(k)], outer_step.at[rows(rep, k)], ss_sem,
                      sr_sem.at[d - 1, k], "rep", rep_peer(d))

    def update_chunk(k, carry):
        a = pltpu.make_async_copy(pseudo.at[0, rows(rep, k)], la, ld_sem.at[0])
        m = pltpu.make_async_copy(momentum.at[part(k)], mom, ld_sem.at[2])
        a.start()
        m.start()
        exchange(0, k).wait_recv()
        b = pltpu.make_async_copy(xch.at[0, part(k)], lb, ld_sem.at[1])
        b.start()
        for d in range(1, n_x):
            partial_send(d, k).wait_recv()

        @pl.when(k > 0)
        def _():
            store_momentum(k - 1).wait()

        a.wait()
        b.wait()
        m.wait()

        def update(i, c):
            r = pl.ds(pl.multiple_of(i * row_unit, row_unit), row_unit)
            o = pl.ds(pl.multiple_of(k * chunk + i * row_unit, row_unit), row_unit)
            total = la[r, :].astype(f32) + lb[r, :].astype(f32)
            for d in range(1, n_x):
                total += pr[d - 1, o, :].astype(f32)
            average = total / n_rep
            fresh = momentum_rate * mom[r, :] + average
            nmb[r, :] = fresh
            pr[0, o, :] = (outer_rate * (average + momentum_rate * fresh)).astype(bf16)
            return c

        lax.fori_loop(0, chunk // row_unit, update, 0)
        for d in range(1, n_x):
            step_send(d, k).start()
        remote(pr.at[0, part(k)], outer_step.at[rows(rep, k)], fs_sem, fr_sem,
               "rep", partner).start()
        pltpu.make_async_copy(pr.at[0, part(k)], outer_step.at[rows(rep, k)], own_sem).start()
        store_momentum(k).start()
        return carry

    lax.fori_loop(0, n_k, update_chunk, 0)
    store_momentum(n_k - 1).wait()

    def forward_chunk(k, carry):
        for d in range(1, n_x):
            step_send(d, k).wait_recv()
            r = rows(2 * chip(n_x - d) + core, k)
            remote(outer_step.at[r], outer_step.at[r], fs_sem, fr_sem, "rep", partner).start()
        return carry

    lax.fori_loop(0, n_k // 2, forward_chunk, 0)

    for d in range(1, n_tp):
        out_send(d).wait()

    def sum_out(i, carry):
        r = pl.ds(pl.multiple_of(i * row_unit, row_unit), row_unit)
        o = pl.ds(pl.multiple_of(tp * t_rows + i * row_unit, row_unit), row_unit)
        total = po[o, :].astype(f32)
        for d in range(1, n_tp):
            total += tr[d - 1, r, :].astype(f32)
        tr[0, r, :] = total.astype(bf16)
        return carry

    lax.fori_loop(0, t_rows // row_unit, sum_out, 0)
    out_copy = pltpu.make_async_copy(tr.at[0], layer_out.at[0], ld_sem.at[0])
    out_copy.start()

    for d in range(1, n_dp):
        drain(dr.at[d - 1], dr_sem.at[d - 1])

    def sum_back(f, carry):
        c = pl.ds(pl.multiple_of(f * fb, fb), fb)

        def band(i, z):
            r = pl.ds(pl.multiple_of(i * row_unit, row_unit), row_unit)
            o = pl.ds(pl.multiple_of(dp * d_rows + i * row_unit, row_unit), row_unit)
            total = pb[o, c].astype(f32)
            for d in range(1, n_dp):
                total += dr[d - 1, r, c].astype(f32)
            dr[0, r, c] = total.astype(bf16)
            return z

        lax.fori_loop(0, d_rows // row_unit, band, 0)
        return carry

    lax.fori_loop(0, n_f, sum_back, 0)
    back_copy = pltpu.make_async_copy(dr.at[0], hidden_grad.at[0], ld_sem.at[1])
    back_copy.start()

    lax.fori_loop(n_k // 2, n_k, forward_chunk, 0)

    out_copy.wait()
    back_copy.wait()
    drain(xch, xs_sem)
    drain(ps, ps_sem)
    drain(ps, ss_sem)
    drain(xch, fs_sem)
    drain(xch, fr_sem)
    drain(pr.at[0], own_sem)
    drain(dr, ds_sem)


def per_device(sizes, hidden, down_weight, out_grad, pseudo_grad, momentum):
    n_rep, n_dp, n_tp = sizes
    n_x = n_rep // 2
    tokens = hidden.shape[1]
    ffn, cols = down_weight.shape
    share = momentum.shape[0]
    n_k = pieces(share, 16, 14)
    n_f = pieces(ffn, 128, 14)
    chunk, fb = share // n_k, ffn // n_f
    t_rows, d_rows = tokens // n_tp, tokens // n_dp
    dma = pltpu.SemaphoreType.DMA
    out = pl.pallas_call(
        functools.partial(kernel, n_rep, n_dp, n_tp, n_k, n_f),
        out_shape=(
            jax.ShapeDtypeStruct((1, t_rows, cols), bf16),
            jax.ShapeDtypeStruct((1, d_rows, ffn), bf16),
            jax.ShapeDtypeStruct((share, cols), f32),
            jax.ShapeDtypeStruct((ffn, cols), bf16),
            jax.ShapeDtypeStruct((n_x, share, cols), bf16),
        ),
        in_specs=[pl.BlockSpec(memory_space=pl.ANY)] * 5,
        out_specs=[pl.BlockSpec(memory_space=pl.ANY)] * 5,
        scratch_shapes=[
            pltpu.VMEM((n_x - 1, share, cols), bf16),
            pltpu.VMEM((n_x - 1, share, cols), bf16),
            pltpu.VMEM((chunk, cols), bf16),
            pltpu.VMEM((chunk, cols), bf16),
            pltpu.VMEM((chunk, cols), f32),
            pltpu.VMEM((chunk, cols), f32),
            pltpu.VMEM((fb, cols), bf16),
            pltpu.VMEM((tokens, fb), bf16),
            pltpu.VMEM((tokens, cols), bf16),
            pltpu.VMEM((tokens, cols), f32),
            pltpu.VMEM((tokens, cols), bf16),
            pltpu.VMEM((n_tp - 1, t_rows, cols), bf16),
            pltpu.VMEM((tokens, ffn), bf16),
            pltpu.VMEM((n_dp - 1, d_rows, ffn), bf16),
            dma((4,)),
            dma,
            dma((n_x, n_k)),
            dma,
            dma((n_x - 1, n_k)),
            dma,
            dma((n_x - 1, n_k)),
            dma,
            dma,
            dma,
            dma((n_tp - 1,)),
            dma((n_tp - 1,)),
            dma((n_tp - 1,)),
            dma((n_tp - 1,)),
            dma,
            dma((n_dp - 1,)),
        ],
        compiler_params=pltpu.CompilerParams(
            collective_id=0, has_side_effects=True, vmem_limit_bytes=60 * 2**20
        ),
        name="layer_step",
    )(hidden, down_weight, out_grad, pseudo_grad, momentum)
    return out[:4]


def solution(mesh):
    sizes = tuple(mesh.shape[a] for a in ("rep", "dp", "tp"))
    return jax.shard_map(
        functools.partial(per_device, sizes),
        mesh=mesh,
        in_specs=(
            P("rep", None, "tp"),
            P("tp", "dp"),
            P("rep", "tp", "dp"),
            P("rep", "tp", "dp"),
            P(("tp", "rep"), "dp"),
        ),
        out_specs=(
            P("rep", "tp", "dp"),
            P("rep", "dp", "tp"),
            P(("tp", "rep"), "dp"),
            P("tp", "dp"),
        ),
        check_vma=False,
    )
```

```python
import functools

import jax
import jax.numpy as jnp
from jax import lax
from jax.experimental import pallas as pl
from jax.experimental.pallas import tpu as pltpu
from jax.sharding import PartitionSpec as P

outer_rate = 0.7
momentum_rate = 0.9

MESH = pl.DeviceIdType.MESH
f32 = jnp.float32
bf16 = jnp.bfloat16


def pieces(extent, unit, most):
    return max(k for k in range(1, most + 1) if extent % (k * unit) == 0)


def kernel(
    n_rep, n_dp, n_tp, n_k, n_late, n_f,
    hidden, weight, grads, pseudo, momentum,
    layer_out, hidden_grad, new_momentum, outer_step, late, xch,
    ps, pr, la, lb, mom, nmb, wb, hb, gf, acc, po, tr, pb, dr,
    ld_sem, xs_sem, xr_sem, ps_sem, pr_sem, ss_sem, sr_sem, fs_sem, fr_sem, own_sem,
    gs_sem, gr_sem, ts_sem, tr_sem, ds_sem, dr_sem,
):
    n_x = n_rep // 2
    rep, dp, tp = lax.axis_index("rep"), lax.axis_index("dp"), lax.axis_index("tp")
    x, core = rep // 2, lax.rem(rep, 2)
    partner = 2 * x + 1 - core
    share, cols = momentum.shape
    chunk = share // n_k
    ffn = weight.shape[0]
    fb = ffn // n_f
    tokens = hidden.shape[1]
    t_rows, d_rows = tokens // n_tp, tokens // n_dp
    row_unit = 16
    n_sent = n_k - n_late
    sent = pl.ds(0, n_sent * chunk)

    def chip(d):
        return lax.rem(x + d, n_x)

    def rep_peer(d):
        return 2 * chip(d) + core

    def rows(owner, k):
        return pl.ds(pl.multiple_of(owner * share + k * chunk, chunk), chunk)

    def part(k):
        return pl.ds(pl.multiple_of(k * chunk, chunk), chunk)

    def remote(src, dst, send, recv, axis, index):
        return pltpu.make_async_remote_copy(
            src_ref=src, dst_ref=dst, send_sem=send, recv_sem=recv,
            device_id={axis: index}, device_id_type=MESH,
        )

    def drain(ref, sem):
        pltpu.make_async_copy(ref, ref, sem).wait()

    barrier = pltpu.get_barrier_semaphore()
    peers = [("rep", partner)]
    peers += [("rep", rep_peer(d)) for d in range(1, n_x)]
    peers += [("dp", lax.rem(dp + d, n_dp)) for d in range(1, n_dp)]
    peers += [("tp", lax.rem(tp + d, n_tp)) for d in range(1, n_tp)]
    for axis, index in peers:
        pl.semaphore_signal(barrier, inc=1, device_id={axis: index}, device_id_type=MESH)
    pl.semaphore_wait(barrier, len(peers))

    def exchange(d, k):
        return remote(
            pseudo.at[0, rows(2 * chip(d) + 1 - core, k)], xch.at[d, part(k)],
            xs_sem, xr_sem.at[d, k], "rep", partner,
        )

    def start_exchange(k, carry):
        for d in range(1, n_x):
            exchange(d, k).start()
        return carry

    def start_own_exchange(k, carry):
        exchange(0, k).start()
        return carry

    lax.fori_loop(0, n_k, start_exchange, 0)

    mine = pl.ds(pl.multiple_of(tp * t_rows, t_rows), t_rows)

    def gather(d):
        return remote(grads.at[0], gf.at[mine], gs_sem.at[d - 1], gr_sem.at[d - 1],
                      "tp", lax.rem(tp + d, n_tp))

    for d in range(1, n_tp):
        gather(d).start()
    own_grads = pltpu.make_async_copy(grads.at[0], gf.at[mine], own_sem)
    own_grads.start()
    lax.fori_loop(0, n_k, start_own_exchange, 0)

    def partial_send(d, k):
        return remote(ps.at[d - 1, part(k)], pr.at[d - 1, part(k)], ps_sem,
                      pr_sem.at[d - 1, k], "rep", rep_peer(d))

    def reduce_chunk(k, carry):
        for d in range(1, n_x):
            a = pltpu.make_async_copy(pseudo.at[0, rows(rep_peer(d), k)], la, ld_sem.at[0])
            a.start()
            exchange(d, k).wait_recv()
            b = pltpu.make_async_copy(xch.at[d, part(k)], lb, ld_sem.at[1])
            b.start()
            a.wait()
            b.wait()

            def add(i, c):
                r = pl.ds(pl.multiple_of(i * row_unit, row_unit), row_unit)
                o = pl.ds(pl.multiple_of(k * chunk + i * row_unit, row_unit), row_unit)
                ps[d - 1, o, :] = (la[r, :].astype(f32) + lb[r, :].astype(f32)).astype(bf16)
                return c

            lax.fori_loop(0, chunk // row_unit, add, 0)
            partial_send(d, k).start()
        return carry

    lax.fori_loop(0, n_k, reduce_chunk, 0)

    tn = cols // pieces(cols, 128, max(1, cols // 512))
    tm = tokens // pieces(tokens, row_unit, 2)

    def clear(i, carry):
        r = pl.ds(pl.multiple_of(i * row_unit, row_unit), row_unit)
        acc[r, :] = jnp.zeros((row_unit, cols), f32)
        return carry

    lax.fori_loop(0, tokens // row_unit, clear, 0)
    own_grads.wait()
    for d in range(1, n_tp):
        gather(d).wait()

    def back_send(d, f):
        to = lax.rem(dp + d, n_dp)
        c = pl.ds(pl.multiple_of(f * fb, fb), fb)
        return remote(
            pb.at[pl.ds(pl.multiple_of(to * d_rows, d_rows), d_rows), c],
            dr.at[d - 1, :, c], ds_sem, dr_sem.at[d - 1], "dp", to,
        )

    def matmul_block(f, carry):
        c = pl.ds(pl.multiple_of(f * fb, fb), fb)
        a = pltpu.make_async_copy(weight.at[c], wb, ld_sem.at[0])
        b = pltpu.make_async_copy(hidden.at[0, :, c], hb, ld_sem.at[1])
        a.start()
        b.start()
        a.wait()
        b.wait()

        def back(m, z):
            r = pl.ds(pl.multiple_of(m * tm, tm), tm)
            product = lax.dot_general(
                gf[r, :], wb[...], (((1,), (1,)), ((), ())), preferred_element_type=f32
            )
            pb[r, c] = product.astype(bf16)
            return z

        lax.fori_loop(0, tokens // tm, back, 0)
        for d in range(1, n_dp):
            back_send(d, f).start()

        def forward(n, z):
            t = pl.ds(pl.multiple_of(n * tn, tn), tn)
            acc[:, t] += jnp.dot(hb[...], wb[:, t], preferred_element_type=f32)
            return z

        lax.fori_loop(0, cols // tn, forward, 0)
        return carry

    lax.fori_loop(0, n_f, matmul_block, 0)

    def round_out(i, carry):
        r = pl.ds(pl.multiple_of(i * row_unit, row_unit), row_unit)
        po[r, :] = acc[r, :].astype(bf16)
        return carry

    lax.fori_loop(0, tokens // row_unit, round_out, 0)

    def out_send(d):
        to = lax.rem(tp + d, n_tp)
        return remote(po.at[pl.ds(pl.multiple_of(to * t_rows, t_rows), t_rows)],
                      tr.at[d - 1], ts_sem.at[d - 1], tr_sem.at[d - 1], "tp", to)

    for d in range(1, n_tp):
        out_send(d).start()

    def store_momentum(k):
        return pltpu.make_async_copy(nmb, new_momentum.at[part(k)], ld_sem.at[3])

    def step_send(d, k):
        return remote(pr.at[0, part(k)], outer_step.at[rows(rep, k)], ss_sem,
                      sr_sem.at[d - 1, k], "rep", rep_peer(d))

    def update_chunk(k, carry):
        a = pltpu.make_async_copy(pseudo.at[0, rows(rep, k)], la, ld_sem.at[0])
        m = pltpu.make_async_copy(momentum.at[part(k)], mom, ld_sem.at[2])
        a.start()
        m.start()
        exchange(0, k).wait_recv()
        b = pltpu.make_async_copy(xch.at[0, part(k)], lb, ld_sem.at[1])
        b.start()
        for d in range(1, n_x):
            partial_send(d, k).wait_recv()

        @pl.when(k > 0)
        def _():
            store_momentum(k - 1).wait()

        a.wait()
        b.wait()
        m.wait()

        def update(i, c):
            r = pl.ds(pl.multiple_of(i * row_unit, row_unit), row_unit)
            o = pl.ds(pl.multiple_of(k * chunk + i * row_unit, row_unit), row_unit)
            total = la[r, :].astype(f32) + lb[r, :].astype(f32)
            for d in range(1, n_x):
                total += pr[d - 1, o, :].astype(f32)
            average = total / n_rep
            fresh = momentum_rate * mom[r, :] + average
            nmb[r, :] = fresh
            pr[0, o, :] = (outer_rate * (average + momentum_rate * fresh)).astype(bf16)
            return c

        lax.fori_loop(0, chunk // row_unit, update, 0)

        @pl.when(k < n_sent)
        def _():
            for d in range(1, n_x):
                step_send(d, k).start()
            remote(pr.at[0, part(k)], outer_step.at[rows(rep, k)], fs_sem, fr_sem,
                   "rep", partner).start()
            pltpu.make_async_copy(
                pr.at[0, part(k)], outer_step.at[rows(rep, k)], own_sem
            ).start()

        store_momentum(k).start()
        return carry

    lax.fori_loop(0, n_k, update_chunk, 0)
    store_momentum(n_k - 1).wait()
    late_copy = pltpu.make_async_copy(
        pr.at[0, pl.ds(n_sent * chunk, n_late * chunk)], late, ld_sem.at[3]
    )
    late_copy.start()

    def forward_chunk(k, carry):
        for d in range(1, n_x):
            step_send(d, k).wait_recv()
            r = rows(2 * chip(n_x - d) + core, k)
            remote(outer_step.at[r], outer_step.at[r], fs_sem, fr_sem, "rep", partner).start()
        return carry

    lax.fori_loop(0, n_sent // 2, forward_chunk, 0)

    for d in range(1, n_tp):
        out_send(d).wait()

    def sum_out(i, carry):
        r = pl.ds(pl.multiple_of(i * row_unit, row_unit), row_unit)
        o = pl.ds(pl.multiple_of(tp * t_rows + i * row_unit, row_unit), row_unit)
        total = po[o, :].astype(f32)
        for d in range(1, n_tp):
            total += tr[d - 1, r, :].astype(f32)
        tr[0, r, :] = total.astype(bf16)
        return carry

    lax.fori_loop(0, t_rows // row_unit, sum_out, 0)
    out_copy = pltpu.make_async_copy(tr.at[0], layer_out.at[0], ld_sem.at[0])
    out_copy.start()

    for d in range(1, n_dp):
        drain(dr.at[d - 1], dr_sem.at[d - 1])

    def sum_back(f, carry):
        c = pl.ds(pl.multiple_of(f * fb, fb), fb)

        def band(i, z):
            r = pl.ds(pl.multiple_of(i * row_unit, row_unit), row_unit)
            o = pl.ds(pl.multiple_of(dp * d_rows + i * row_unit, row_unit), row_unit)
            total = pb[o, c].astype(f32)
            for d in range(1, n_dp):
                total += dr[d - 1, r, c].astype(f32)
            dr[0, r, c] = total.astype(bf16)
            return z

        lax.fori_loop(0, d_rows // row_unit, band, 0)
        return carry

    lax.fori_loop(0, n_f, sum_back, 0)
    back_copy = pltpu.make_async_copy(dr.at[0], hidden_grad.at[0], ld_sem.at[1])
    back_copy.start()

    lax.fori_loop(n_sent // 2, n_sent, forward_chunk, 0)

    out_copy.wait()
    back_copy.wait()
    late_copy.wait()
    drain(xch, xs_sem)
    drain(ps, ps_sem)
    drain(ps.at[:, sent], ss_sem)
    drain(xch.at[:, sent], fs_sem)
    drain(xch.at[:, sent], fr_sem)
    drain(pr.at[0, sent], own_sem)
    drain(dr, ds_sem)


def copy_bands(*refs):
    half = len(refs) // 2
    for source, target in zip(refs[:half], refs[half:]):
        target[...] = source[...]


def per_device(sizes, hidden, down_weight, out_grad, pseudo_grad, momentum):
    n_rep, n_dp, n_tp = sizes
    n_x = n_rep // 2
    tokens = hidden.shape[1]
    ffn, cols = down_weight.shape
    share = momentum.shape[0]
    n_k = pieces(share, 16, 14)
    n_f = pieces(ffn, 128, 14)
    n_late = max(1, n_k // 7)
    chunk, fb = share // n_k, ffn // n_f
    late_rows = n_late * chunk
    t_rows, d_rows = tokens // n_tp, tokens // n_dp
    dma = pltpu.SemaphoreType.DMA
    out = pl.pallas_call(
        functools.partial(kernel, n_rep, n_dp, n_tp, n_k, n_late, n_f),
        out_shape=(
            jax.ShapeDtypeStruct((1, t_rows, cols), bf16),
            jax.ShapeDtypeStruct((1, d_rows, ffn), bf16),
            jax.ShapeDtypeStruct((share, cols), f32),
            jax.ShapeDtypeStruct((ffn, cols), bf16),
            jax.ShapeDtypeStruct((late_rows, cols), bf16),
            jax.ShapeDtypeStruct((n_x, share, cols), bf16),
        ),
        in_specs=[pl.BlockSpec(memory_space=pl.ANY)] * 5,
        out_specs=[pl.BlockSpec(memory_space=pl.ANY)] * 6,
        scratch_shapes=[
            pltpu.VMEM((n_x - 1, share, cols), bf16),
            pltpu.VMEM((n_x - 1, share, cols), bf16),
            pltpu.VMEM((chunk, cols), bf16),
            pltpu.VMEM((chunk, cols), bf16),
            pltpu.VMEM((chunk, cols), f32),
            pltpu.VMEM((chunk, cols), f32),
            pltpu.VMEM((fb, cols), bf16),
            pltpu.VMEM((tokens, fb), bf16),
            pltpu.VMEM((tokens, cols), bf16),
            pltpu.VMEM((tokens, cols), f32),
            pltpu.VMEM((tokens, cols), bf16),
            pltpu.VMEM((n_tp - 1, t_rows, cols), bf16),
            pltpu.VMEM((tokens, ffn), bf16),
            pltpu.VMEM((n_dp - 1, d_rows, ffn), bf16),
            dma((4,)),
            dma,
            dma((n_x, n_k)),
            dma,
            dma((n_x - 1, n_k)),
            dma,
            dma((n_x - 1, n_k)),
            dma,
            dma,
            dma,
            dma((n_tp - 1,)),
            dma((n_tp - 1,)),
            dma((n_tp - 1,)),
            dma((n_tp - 1,)),
            dma,
            dma((n_dp - 1,)),
        ],
        compiler_params=pltpu.CompilerParams(
            collective_id=0, has_side_effects=True, vmem_limit_bytes=60 * 2**20
        ),
        name="layer_step",
    )(hidden, down_weight, out_grad, pseudo_grad, momentum)
    layer_out, hidden_grad, new_momentum, outer_step, late = out[:5]
    late = lax.all_gather(late, "rep", axis=0, tiled=False)
    results = (layer_out, hidden_grad, new_momentum, outer_step)
    steps = max(
        k for k in range(1, 9)
        if not any(n % (16 * k) for n in (t_rows, d_rows, ffn)) and share % (8 * k) == 0
    )

    def band(array):
        block = array.shape[:-2] + (array.shape[-2] // steps, array.shape[-1])
        return pl.BlockSpec(block, lambda i: (0,) * (array.ndim - 2) + (i, 0))

    layer_out, hidden_grad, new_momentum, outer_step = pl.pallas_call(
        copy_bands,
        out_shape=tuple(jax.ShapeDtypeStruct(r.shape, r.dtype) for r in results),
        grid=(steps,),
        in_specs=[band(r) for r in results],
        out_specs=[band(r) for r in results],
        cost_estimate=pl.CostEstimate(
            flops=0, bytes_accessed=2 * sum(r.nbytes for r in results), transcendentals=0
        ),
        compiler_params=pltpu.CompilerParams(vmem_limit_bytes=40 * 2**20),
        name="result_copy",
    )(*results)
    outer_step = lax.dynamic_update_slice(
        outer_step.reshape(n_rep, share, cols), late, (0, share - late_rows, 0)
    ).reshape(ffn, cols)
    return layer_out, hidden_grad, new_momentum, outer_step


def solution(mesh):
    sizes = tuple(mesh.shape[a] for a in ("rep", "dp", "tp"))
    return jax.shard_map(
        functools.partial(per_device, sizes),
        mesh=mesh,
        in_specs=(
            P("rep", None, "tp"),
            P("tp", "dp"),
            P("rep", "tp", "dp"),
            P("rep", "tp", "dp"),
            P(("tp", "rep"), "dp"),
        ),
        out_specs=(
            P("rep", "tp", "dp"),
            P("rep", "dp", "tp"),
            P(("tp", "rep"), "dp"),
            P("tp", "dp"),
        ),
        check_vma=False,
    )
```
